256 devices in a mesh: img: 64 (over y, z, core), nrn: 4 (over x).
Axes of the slice: x: 4, y: 4, z: 8, core: 2. Of those that a mesh axis runs over, the one named last changes fastest.
Arguments:
- images: bfloat16 [16384, 16384], P('img', 'nrn'), may hold values from 0 to 12
- weights: bfloat16 [2, 128, 512, 128], P(None, 'nrn'), may hold values from -0.375 to 0.375
- block_index: int32 [2, 128, 4], replicated, may hold values from 0 to 127, as said below
- bias: float32 [2, 16384], replicated, may hold values from -0.2 to -0.02
Outputs:
- activations: bfloat16 [16384, 16384], P('img', 'nrn')
- live_fraction: float32 [2], replicated
The draws below stay inside these ranges and needn't reach their ends.
Inputs may be any that keep to these rules, and one draw needn't show every extreme that they name: `block_index`: the 4 entries of each row name different blocks.
All inputs are finite; a program needn't handle non-finite values.
Results may differ from the reference program's by a relative error of at most 0.005.
Values may be sent and summed in bfloat16 or wider, within the bound.
A program may use at most 128 MiB of HBM per device.

```python
import math
import jax
import jax.numpy as jnp
from jax import lax

NEURONS = 16384
TILE = 128
K = 4
LAYERS = 2
IMG_GRP = 256
BLOCKS = 128
N_IMG = 64


def draw_images(key, part):
    first, second, third = jax.random.split(key, 3)
    total_rows = IMG_GRP * N_IMG
    positions = jnp.arange(total_rows, dtype=jnp.float32)
    ramp = 1.0 + 2.0 * positions / max(total_rows - 1, 1)
    scales = jnp.exp(jax.random.uniform(first, (total_rows, 1), jnp.float32, math.log(0.25), 0.0)) * ramp[:, None]
    base = jnp.abs(jax.random.normal(second, (total_rows, NEURONS), jnp.float32))
    keeper = jax.random.bernoulli(third, 0.5, (total_rows, NEURONS)).astype(jnp.float32)
    values = jnp.minimum(base * keeper * scales, 12.0)
    return values.astype(jnp.bfloat16)


def draw_block_index(key, part):
    blocks = NEURONS // TILE
    scores = jax.random.randint(key, (LAYERS, blocks, blocks), 0, 1 << 20, jnp.int32)
    scores = scores * blocks + jnp.arange(blocks, dtype=jnp.int32)
    picked = jax.lax.top_k(scores, K)[1]
    return picked.astype(jnp.int32)


def block_scale(own_key, dims, pieces, smallest, high):
    loudness = 1.0
    for position, parts in pieces:
        draws = jax.random.uniform(jax.random.fold_in(jax.random.fold_in(own_key, 6), position), (parts,), jnp.float32, smallest / len(pieces), high / len(pieces))
        loudness = loudness * jnp.repeat(jnp.exp(draws), dims[position] // parts).reshape((-1,) + (1,) * (len(dims) - 1 - position))
    return loudness


def gaussian(stream_key, dims, width, reach, shards=(), kind=jnp.bfloat16):
    array = width * jax.random.normal(stream_key, dims, jnp.float32)
    if shards:
        array = array * block_scale(stream_key, dims, shards, -0.22, 0.18)
    return jnp.clip(array, -reach, reach).astype(kind)


def setup_inputs(seed: int = 0) -> dict:
    splits = jax.random.split(jax.random.key(seed), 5)
    images = draw_images(jax.random.fold_in(splits[4], 71), 0)
    weights = gaussian(splits[1], (LAYERS, BLOCKS, K * TILE, TILE), (K * TILE // 2) ** -0.5, 0.375, ((1, 4),))
    block_index = draw_block_index(jax.random.fold_in(splits[4], 71), 0)
    bias = jnp.clip(jax.random.uniform(splits[3], (LAYERS, NEURONS), jnp.float32, -0.2, -0.02), -0.2, -0.02)
    return dict(images=images, weights=weights, block_index=block_index, bias=bias)


live_level = 0.25


def reference(images, weights, block_index, bias):
    blocks = NEURONS // TILE
    current = images
    live_terms = []
    for layer_no in range(LAYERS):
        tiles = weights[layer_no].astype(jnp.float32)
        chosen = block_index[layer_no].reshape(-1).astype(jnp.int32)
        offsets = bias[layer_no]

        def apply_layer(batch_rows):
            count = batch_rows.shape[0]
            blocked = batch_rows.reshape(count, blocks, TILE)
            picked = jnp.take(blocked, chosen, axis=1).reshape(count, blocks, K * TILE).astype(jnp.float32)
            result = jnp.einsum("brk,rkc->brc", picked, tiles, precision=lax.Precision.HIGHEST)
            result = result.reshape(count, NEURONS) + offsets
            return jnp.maximum(result, 0.0).astype(jnp.bfloat16)

        current = lax.map(apply_layer, current.reshape(N_IMG, IMG_GRP, NEURONS)).reshape(N_IMG * IMG_GRP, NEURONS)
        means = jnp.sum(current.astype(jnp.float32), axis=1) / NEURONS
        live_terms.append(jnp.sum(jnp.minimum(1.0, means / live_level)) / (N_IMG * IMG_GRP))
    return current, jnp.stack(live_terms)
```

```python
import jax
import jax.numpy as jnp
from jax import lax
from jax.experimental import pallas as pl
from jax.experimental.pallas import tpu as pltpu
from jax.sharding import PartitionSpec as P

MESH = pl.DeviceIdType.MESH
LIVE_LEVEL = 0.25
NX, NY, NZ, NW = 4, 4, 8, 4
T = 128


def kernel(img, w, bi, bias, out, stat, im, X, Y1, Wb, Wo, Ob, acc, accr, rz, ry, rx,
           x_ss, x_rs, w_ss, w_rs, y_ss, y_rs, o_ss, o_rs, a_ss, a_rs, l_sem, im_sem, z_ss, z_rs):
    x = lax.axis_index("nrn")
    i = lax.axis_index("img")
    c = i % 2
    z = (i // 2) % NZ
    y = i // (2 * NZ)
    zm = z % NW
    rows = img.shape[0] // NX
    cols = img.shape[1]
    per_x = w.shape[1]
    half = per_x // 2
    kk = w.shape[2]
    hk, qk = kk // 2, kk // 4

    def dev(dx=0, dy=0, dz=0, s=0):
        cc = (c + s) % 2
        return (((y + dy + NY) % NY) * 2 * NZ + ((z + dz + NZ) % NZ) * 2 + cc, (x + dx + NX) % NX)

    def rc(src, dst, ss, rs, d):
        return pltpu.make_async_remote_copy(src_ref=src, dst_ref=dst, send_sem=ss, recv_sem=rs,
                                            device_id=d, device_id_type=MESH)

    partners = [dev(s=1), dev(dy=1), dev(dy=-1), dev(dz=1), dev(dz=-1)]
    partners += [dev(dx=d, s=s) for d in (1, 2, 3) for s in (0, 1)]
    partners += [dev(dz=d) for d in range(2, NZ - 1)] + [dev(dy=2)]
    bar = pltpu.get_barrier_semaphore()
    for p in partners:
        pl.semaphore_signal(bar, 1, device_id=p, device_id_type=MESH)
    pl.semaphore_wait(bar, len(partners))

    def xrow(g):
        return pl.ds(pl.multiple_of(g * rows, rows), rows)

    def xblk(q):
        return pl.ds(q * per_x, per_x)

    def xa_send(d):
        t = (x + d) % NX
        return rc(im.at[:, xrow(t), :], X.at[xblk(x), xrow(c), :], x_ss.at[d], x_rs.at[d], dev(dx=d))

    def xa_recv(d):
        q = (x - d + NX) % NX
        return rc(im.at[:, xrow(x), :], X.at[xblk(q), xrow(c), :], x_ss.at[d], x_rs.at[d], dev(dx=d))

    def xf(d, other=0):
        q = (x - d + NX) % NX
        ref = X.at[xblk(q), xrow((c + other) % 2), :]
        if d == 0 and not other:
            src = im.at[:, xrow(x), :]
        else:
            src = ref
        return rc(src, ref, x_ss.at[3 + d + (d == 0) * 4], x_rs.at[3 + d + (d == 0) * 4], dev(s=1))

    j0 = y * NW + zm

    def xi(l, d):
        return rc(w.at[l, c * half + j0], Wb.at[l, d - 1, 0, 0], w_ss.at[l, d - 1], w_rs.at[l, d - 1], dev(dx=-d))

    def part(l, st, ey, ez, lo, n):
        return Wb.at[l, :, ey, ez, pl.ds(lo, n), :]

    def msgs(l, half_b):
        lo = hk if half_b else 0
        so = 3 + (8 if half_b else 0)
        ro = 3 + (20 if half_b else 0)

        def slot(a, b, lo_, n):
            return part(l, None, b, a, lo_, n) if half_b else part(l, None, a, b, lo_, n)

        up1, dn1 = (dev(dz=1), dev(dz=-1)) if half_b else (dev(dy=1), dev(dy=-1))
        up2, dn2 = (dev(dy=1), dev(dy=-1)) if half_b else (dev(dz=1), dev(dz=-1))
        ws, wr = w_ss, w_rs
        m = {}
        m["1p"] = rc(slot(0, 0, lo, hk), slot(3, 0, lo, hk), ws.at[l, so], wr.at[l, ro], up1)
        m["1m"] = rc(slot(0, 0, lo, hk), slot(1, 0, lo, hk), ws.at[l, so + 1], wr.at[l, ro + 1], dn1)
        m["1fp"] = rc(slot(3, 0, lo, qk), slot(2, 0, lo, qk), ws.at[l, so + 2], wr.at[l, ro + 2], up1)
        m["1fm"] = rc(slot(1, 0, lo + qk, qk), slot(2, 0, lo + qk, qk), ws.at[l, so + 3], wr.at[l, ro + 3], dn1)
        for e in range(4):
            m["2p", e] = rc(slot(e, 0, lo, hk), slot(e, 3, lo, hk), ws.at[l, so + 4], wr.at[l, ro + 4 + e], up2)
            m["2m", e] = rc(slot(e, 0, lo, hk), slot(e, 1, lo, hk), ws.at[l, so + 5], wr.at[l, ro + 8 + e], dn2)
            m["2fp", e] = rc(slot(e, 3, lo, qk), slot(e, 2, lo, qk), ws.at[l, so + 6], wr.at[l, ro + 12 + e], up2)
            m["2fm", e] = rc(slot(e, 1, lo + qk, qk), slot(e, 2, lo + qk, qk), ws.at[l, so + 7], wr.at[l, ro + 16 + e], dn2)
        def allsl(b, lo_, n):
            return Wb.at[l, :, b, :, pl.ds(lo_, n), :] if half_b else Wb.at[l, :, :, b, pl.ds(lo_, n), :]
        m["sends"] = [m["1p"], m["1m"], m["1fp"], m["1fm"]]
        for b, o, n, k in ((0, 0, hk, 4), (0, 0, hk, 5), (3, 0, qk, 6), (1, qk, qk, 7)):
            r = allsl(b, lo + o, n)
            m["sends"].append(rc(r, r, ws.at[l, so + k], wr.at[l, ro + 4], up2))
        return m

    MA = [msgs(l, False) for l in range(2)]
    MB = [msgs(l, True) for l in range(2)]

    def s0(l):
        for d in (1, 3, 2):
            xi(l, d).wait_recv()
        for k in ("1p", "1m", ("2p", 0), ("2m", 0)):
            MA[l][k].start()
            MB[l][k].start()

    def s1(l):
        for k, e in (("p", 3), ("m", 1)):
            MA[l]["1" + k].wait_recv()
            MB[l]["1" + k].wait_recv()
            MA[l]["1f" + k].start()
            MB[l]["1f" + k].start()
        for e in (3, 1):
            for k in ("2p", "2m"):
                MA[l][k, e].start()
                MB[l][k, e].start()

    def s2(l):
        for k in ("1fp", "1fm"):
            MA[l][k].wait_recv()
            MB[l][k].wait_recv()
        for k in ("2p", "2m"):
            MA[l][k, 2].start()
            MB[l][k, 2].start()

    def s3(l, e):
        for k in ("p", "m"):
            MA[l]["2" + k, e].wait_recv()
            MB[l]["2" + k, e].wait_recv()
            MA[l]["2f" + k, e].start()
            MB[l]["2f" + k, e].start()

    def s4(l, e):
        for k in ("2fp", "2fm"):
            MA[l][k, e].wait_recv()
            MB[l][k, e].wait_recv()

    def block(l, q, j, wt, store):
        src = X if l == 0 else Y1
        r = q * per_x + c * half + j
        xs = [src[bi[l, r, k]] for k in range(kk // T)]
        pre = jnp.dot(jnp.concatenate(xs, axis=1), wt, preferred_element_type=jnp.float32)
        pre = pre + bias[pl.ds(l, 1), pl.ds(pl.multiple_of(r * T, T), T)]
        act = jnp.maximum(pre, 0.0).astype(jnp.bfloat16)
        store(r, act)
        return act.astype(jnp.float32)

    def put(l, d, j):
        def store(r, act):
            if l == 0:
                Y1[r] = act
            else:
                Ob[d, :, pl.ds(pl.multiple_of(j * T, T), T)] = act
        return store

    def own_blocks(l):
        def body(t, _):
            s = acc[l]
            for u in range(2):
                j = t * 2 + u
                s = s + block(l, x, j, Wo[l, j], put(l, 0, j))
            acc[l] = s
            return 0
        lax.fori_loop(0, half // 2, body, 0)

    def slots(l, n, fey, fez):
        def body(t, _):
            ey, ez = fey(t), fez(t)
            j = ((y + ey) % NY) * NW + (zm + ez) % NW
            s = acc[l]
            for d in (1, 2, 3):
                s = s + block(l, (x + d) % NX, j, Wb[l, d - 1, ey, ez], put(l, d, j))
            acc[l] = s
            return 0
        lax.fori_loop(0, n, body, 0)

    def osl(q):
        return pl.ds(pl.multiple_of(q * half * T, half * T), half * T)

    def y1x(d, other):
        cc = (c + other) % 2
        q = (x + d) % NX
        ref = Y1.at[pl.ds((q * 2 + cc) * half, half)]
        return rc(ref, ref, y_ss.at[d], y_rs.at[d], dev(s=1))

    def out_send(d, s, j, n=1):
        src = Ob.at[d, xrow((c + s) % 2), pl.ds(pl.multiple_of(j * T, T), n * T)]
        dst = out.at[xrow(x), pl.ds(pl.multiple_of((c * half + j) * T, T), n * T)]
        if d == 0 and s == 0:
            return pltpu.make_async_copy(src, dst, l_sem.at[3])
        return rc(src, dst, o_ss.at[d, s], o_rs.at[d, s], dev(dx=d, s=s))

    def out_wait(d, s, recv):
        if recv:
            ref = out.at[xrow((x - d + NX) % NX), osl((c + s) % 2)]
            rc(ref, ref, o_ss.at[d, s], o_rs.at[d, s], dev(dx=d, s=s)).wait_recv()
        else:
            ref = Ob.at[d, xrow((c + s) % 2), :]
            rc(ref, ref, o_ss.at[d, s], o_rs.at[d, s], dev(dx=d, s=s)).wait_send()

    def send_slots(pairs):
        for ey, ez in pairs:
            j = ((y + ey) % NY) * NW + (zm + ez) % NW
            for d in (1, 3, 2):
                for s in (0, 1):
                    out_send(d, s, j).start()

    for d in (1, 3, 2):
        xi(0, d).start()
    imc = [pltpu.make_async_copy(img.at[:, pl.ds(b * T, T)], im.at[b], im_sem) for b in range(per_x)]
    for cp in imc:
        cp.start()
    pltpu.make_async_copy(im, im, im_sem).wait()
    for d in (1, 3, 2):
        xa_send(d).start()
    xf(0).start()
    for d in (1, 3, 2):
        xi(1, d).start()
    local = [pltpu.make_async_copy(w.at[l, pl.ds(pl.multiple_of(c * half, half), half)], Wo.at[l], l_sem.at[l])
             for l in range(2)]
    local.append(pltpu.make_async_copy(im.at[:, xrow(x), :], X.at[xblk(x), xrow(c), :], l_sem.at[2]))
    for cp in local:
        cp.start()
    acc[...] = jnp.zeros_like(acc)

    s0(0)
    s1(0)
    s3(0, 0)
    s2(0)
    s3(0, 3)
    s3(0, 1)
    for d in (1, 3, 2):
        xa_recv(d).wait_recv()
        xf(d).start()
    s3(0, 2)
    for cp in local:
        cp.wait()
    for d in (0, 1, 3, 2):
        xf(d, other=1).wait_recv()
    s0(1)
    own_blocks(0)
    for e in range(4):
        s4(0, e)
    y1x(0, 0).start()
    slots(0, 4, lambda t: 0, lambda t: t)
    s1(1)
    slots(0, 4, lambda t: 1, lambda t: t)
    s3(1, 0)
    slots(0, 8, lambda t: 2 + t // 4, lambda t: t % 4)
    s2(1)
    for d in (1, 2, 3):
        y1x(d, 0).start()
    s3(1, 3)
    for d in range(4):
        y1x(d, 1).wait_recv()
    own_blocks(1)
    slots(1, 1, lambda t: 0, lambda t: 0)
    s3(1, 1)
    for s in (0, 1):
        out_send(0, s, 0, half).start()
    send_slots([(0, 0)])
    slots(1, 2, lambda t: 0, lambda t: 1 + 2 * t)
    slots(1, 2, lambda t: 1 + 2 * t, lambda t: 0)
    send_slots([(0, 1), (0, 3), (1, 0), (3, 0)])
    s3(1, 2)
    slots(1, 4, lambda t: 1 + 2 * (t // 2), lambda t: 1 + 2 * (t % 2))
    s4(1, 0)
    send_slots([(1, 1), (1, 3), (3, 1), (3, 3)])
    slots(1, 2, lambda t: 2 * t, lambda t: 2 - 2 * t)
    s4(1, 3)
    s4(1, 1)
    send_slots([(0, 2), (2, 0)])
    slots(1, 2, lambda t: 1 + 2 * t, lambda t: 2)
    slots(1, 2, lambda t: 2, lambda t: 1 + 2 * t)
    send_slots([(1, 2), (3, 2), (2, 1), (2, 3)])
    s4(1, 2)
    slots(1, 1, lambda t: 2, lambda t: 2)

    ax = rc(acc.at[:, xrow((c + 1) % 2), :], accr, a_ss.at[0], a_rs.at[0], dev(s=1))
    send_slots([(2, 2)])
    ax.start()
    mine = acc[:, xrow(c), :]
    ax.wait_recv()
    tot = jnp.sum(mine + accr[...], axis=2)
    share = jnp.minimum(1.0, tot * (1.0 / (NX * cols * LIVE_LEVEL)))
    part_sum = jnp.broadcast_to(jnp.sum(share, axis=1, keepdims=True), (2, T))

    def gather_sum(buf, n, me, val, targets, base):
        buf[me] = val
        cps = [rc(buf.at[me], buf.at[me], z_ss.at[base + k], z_rs.at[base + k], t) for k, (t, _) in enumerate(targets)]
        for cp in cps:
            cp.start()
        for k, (_, who) in enumerate(targets):
            rc(buf.at[who], buf.at[who], z_ss.at[base + k], z_rs.at[base + k], dev(s=1)).wait_recv()
        total = buf[0]
        for k in range(1, n):
            total = total + buf[k]
        for cp in cps:
            cp.wait_send()
        return total

    v = gather_sum(rz, NZ, z, part_sum, [(dev(dz=d), (z - d + NZ) % NZ) for d in range(1, NZ)], 0)
    v = gather_sum(ry, NY, y, v, [(dev(dy=d), (y - d + NY) % NY) for d in range(1, NY)], NZ)
    me_x = [(dev(dx=d, s=s), ((x - d + NX) % NX) * 2 + (c + s) % 2) for d in range(NX) for s in (0, 1) if d or s]
    v = gather_sum(rx, 2 * NX, x * 2 + c, v, me_x, NZ + NY)
    stat[...] = v * (1.0 / (NX * rows * 2 * NZ * NY))

    for l in range(2):
        for d in (1, 2, 3):
            xi(l, d).wait_send()
        for cp in MA[l]["sends"] + MB[l]["sends"]:
            cp.wait_send()
    for d in (1, 2, 3):
        xa_send(d).wait_send()
    for d in range(4):
        xf(d).wait_send()
        y1x(d, 0).wait_send()
    ax.wait_send()
    out_send(0, 0, 0, half).wait()
    for d in range(4):
        for s in (0, 1):
            if d or s:
                out_wait(d, s, True)
                out_wait(d, s, False)


def per_device(images, weights, block_index, bias):
    n_img, cols = images.shape
    layers, per_x, kk, _ = weights.shape
    rows = n_img // NX
    half = per_x // 2
    total = cols * NX
    dma = pltpu.SemaphoreType.DMA
    any_ = pl.BlockSpec(memory_space=pl.ANY)
    vm = pl.BlockSpec(memory_space=pltpu.VMEM)
    out, stat = pl.pallas_call(
        kernel,
        out_shape=(jax.ShapeDtypeStruct((n_img, cols), jnp.bfloat16), jax.ShapeDtypeStruct((layers, T), jnp.float32)),
        in_specs=[any_, any_, pl.BlockSpec(memory_space=pltpu.SMEM), vm],
        out_specs=(any_, vm),
        scratch_shapes=[
            pltpu.VMEM((per_x, n_img, T), jnp.bfloat16),
            pltpu.VMEM((total // T, 2 * rows, T), jnp.bfloat16),
            pltpu.VMEM((total // T, 2 * rows, T), jnp.bfloat16),
            pltpu.VMEM((layers, 3, NY, NW, kk, T), jnp.bfloat16),
            pltpu.VMEM((layers, half, kk, T), jnp.bfloat16),
            pltpu.VMEM((NX, 2 * rows, half * T), jnp.bfloat16),
            pltpu.VMEM((layers, 2 * rows, T), jnp.float32),
            pltpu.VMEM((layers, rows, T), jnp.float32),
            pltpu.VMEM((NZ, layers, T), jnp.float32),
            pltpu.VMEM((NY, layers, T), jnp.float32),
            pltpu.VMEM((2 * NX, layers, T), jnp.float32),
            dma((8,)), dma((8,)),
            dma((layers, 19)), dma((layers, 43)),
            dma((4,)), dma((4,)),
            dma((4, 2)), dma((4, 2)),
            dma((1,)), dma((1,)),
            dma((4,)), dma,
            dma((20,)), dma((20,)),
        ],
        compiler_params=pltpu.CompilerParams(collective_id=0, has_side_effects=True, vmem_limit_bytes=60 * 1024 * 1024),
        name="sparse_net",
    )(images, weights, block_index, bias)
    return out, stat[:, 0]


def solution(mesh):
    return jax.shard_map(
        per_device, mesh=mesh,
        in_specs=(P("img", "nrn"), P(None, "nrn", None, None), P(), P()),
        out_specs=(P("img", "nrn"), P()), check_vma=False,
    )
```

```python
import jax
import jax.numpy as jnp
from jax import lax
from jax.experimental import pallas as pl
from jax.experimental.pallas import tpu as pltpu
from jax.sharding import PartitionSpec as P

MESH = pl.DeviceIdType.MESH
LIVE_LEVEL = 0.25
NX, NY, NZ, NW = 4, 4, 8, 4
T = 128


RINGS = {"a0": 0, "b0": 1, "b1": 2, "a1": 3}


def kernel(img, w, bi_hbm, bias_hbm, out, stat, im, X, Y1, Wb, Wo, Ob, acc, accr, rz, ry, rx, bi, bias,
           x_ss, x_rs, xi_ss, xi_rs, far_ss, far_rs, w_ss, w_rs, y_ss, y_rs, o_ss, o_rs, a_ss, a_rs, l_sem, im_sem, z_ss, z_rs):
    x = lax.axis_index("nrn")
    i = lax.axis_index("img")
    c = i % 2
    z = (i // 2) % NZ
    y = i // (2 * NZ)
    zm = z % NW
    rows = img.shape[0] // NX
    cols = img.shape[1]
    per_x = w.shape[1]
    half = per_x // 2
    kk = w.shape[2]

    def dev(dx=0, dy=0, dz=0, s=0):
        cc = (c + s) % 2
        return (((y + dy + NY) % NY) * 2 * NZ + ((z + dz + NZ) % NZ) * 2 + cc, (x + dx + NX) % NX)

    def rc(src, dst, ss, rs, d):
        return pltpu.make_async_remote_copy(src_ref=src, dst_ref=dst, send_sem=ss, recv_sem=rs,
                                            device_id=d, device_id_type=MESH)

    partners = [dev(dx=d, s=s) for d in (2, 1, 3) for s in (0, 1)]
    partners += [dev(dz=1), dev(dz=-1), dev(dy=1), dev(dy=-1), dev(s=1)]
    bar = pltpu.get_barrier_semaphore()
    for p in partners:
        pl.semaphore_signal(bar, 1, device_id=p, device_id_type=MESH)
    imc = [pltpu.make_async_copy(img.at[:, pl.ds(b * T, T)], im.at[b], im_sem) for b in range(per_x)]
    local = [pltpu.make_async_copy(bi_hbm, bi, l_sem.at[2]), pltpu.make_async_copy(bias_hbm, bias, l_sem.at[4])]
    local += [pltpu.make_async_copy(w.at[l, pl.ds(pl.multiple_of(c * half, half), half)], Wo.at[l], l_sem.at[l])
              for l in range(2)]
    for cp in imc + local:
        cp.start()
    pl.semaphore_wait(bar, len(partners))

    def xrow(g):
        return pl.ds(pl.multiple_of(g * rows, rows), rows)

    def xblk(q):
        return pl.ds(q * per_x, per_x)

    def xa_send(d):
        t = (x + d) % NX
        return rc(im.at[:, xrow(t), :], X.at[xblk(x), xrow(c), :], x_ss.at[d], x_rs.at[d], dev(dx=d))

    def xa_recv(d):
        q = (x - d + NX) % NX
        return rc(im.at[:, xrow(x), :], X.at[xblk(q), xrow(c), :], x_ss.at[d], x_rs.at[d], dev(dx=d))

    def xf(d, other=0):
        q = (x - d + NX) % NX
        ref = X.at[xblk(q), xrow((c + other) % 2), :]
        src = im.at[:, xrow(x), :] if d == 0 and not other else ref
        k = 4 + d
        return rc(src, ref, x_ss.at[k], x_rs.at[k], dev(s=1))

    j0 = y * NW + zm

    def place(ey, ez):
        return ((y + ey) % NY) * NW + (zm + ez) % NW

    def xi(l, d):
        return rc(Wo.at[l, j0], Wb.at[l, d - 1, 0, 0], xi_ss.at[l, d - 1], xi_rs.at[l, d - 1], dev(dx=-d))

    FAR = ((2, 0), (2, 2), (0, 2), (1, 2), (3, 2))

    def far(h, k):
        a, b = FAR[k]
        d = (1, 3)[h]
        ey, ez = (b, a) if h else (a, b)
        return rc(Wo.at[1, place(ey, ez)], Wb.at[1, d - 1, ey, ez], far_ss.at[h, k], far_rs.at[h, k], dev(dx=-d))

    def ring(name):
        n, l = RINGS[name], int(name[1])
        halves = []
        for h in (0, 1):
            if name[0] == "a":
                d, lo, size = (1, 3)[h], 0, kk
            else:
                d, lo, size = 2, h * (kk // 2), kk // 2
            q = size // 2

            def slot(a, b, off, m, d=d, h=h, lo=lo):
                ey, ez = (b, a) if h else (a, b)
                return Wb.at[l, d - 1, ey, ez, pl.ds(lo + off, m), :]

            up1, dn1, up2, dn2 = dev(dy=1), dev(dy=-1), dev(dz=1), dev(dz=-1)
            if h:
                up1, dn1, up2, dn2 = up2, dn2, up1, dn1
            ss, rs = w_ss.at[n, h], w_rs.at[n, h]
            m = {}
            m["1p"] = rc(slot(0, 0, 0, size), slot(3, 0, 0, size), ss.at[0], rs.at[0], up1)
            m["1m"] = rc(slot(0, 0, 0, size), slot(1, 0, 0, size), ss.at[1], rs.at[1], dn1)
            m["1fp"] = rc(slot(3, 0, 0, q), slot(2, 0, 0, q), ss.at[2], rs.at[2], up1)
            m["1fm"] = rc(slot(1, 0, q, q), slot(2, 0, q, q), ss.at[3], rs.at[3], dn1)
            for e in range(4):
                m["2p", e] = rc(slot(e, 0, 0, size), slot(e, 3, 0, size), ss.at[4], rs.at[4 + e], up2)
                m["2m", e] = rc(slot(e, 0, 0, size), slot(e, 1, 0, size), ss.at[5], rs.at[8 + e], dn2)
                m["2fp", e] = rc(slot(e, 3, 0, q), slot(e, 2, 0, q), ss.at[6], rs.at[12 + e], up2)
                m["2fm", e] = rc(slot(e, 1, q, q), slot(e, 2, q, q), ss.at[7], rs.at[16 + e], dn2)
            sends = [m["1p"], m["1m"], m["1fp"], m["1fm"]]
            for k, b, off, size_k in ((4, 0, 0, size), (5, 0, 0, size), (6, 3, 0, q), (7, 1, q, q)):
                r = slot(slice(None), b, off, size_k)
                sends.append(rc(r, r, ss.at[k], rs.at[4], up2))
            m["sends"] = sends[:2] + sends[4:6] if name == "a1" else sends
            halves.append(m)
        return halves

    R = {name: ring(name) for name in RINGS}

    def t0(name):
        for d in (1, 3) if name[0] == "a" else (2,):
            xi(int(name[1]), d).wait_recv()
        for k in ("1p", "1m", ("2p", 0), ("2m", 0)):
            for m in R[name]:
                m[k].start()

    def t1(name):
        for k in "pm":
            for m in R[name]:
                m["1" + k].wait_recv()
            for m in R[name]:
                m["1f" + k].start()
        for e in (3, 1):
            for k in ("2p", "2m"):
                for m in R[name]:
                    m[k, e].start()

    def t2(name):
        for k in ("1fp", "1fm"):
            for m in R[name]:
                m[k].wait_recv()
        for k in ("2p", "2m"):
            for m in R[name]:
                m[k, 2].start()

    def t3(name, e):
        for k in "pm":
            for m in R[name]:
                m["2" + k, e].wait_recv()
            for m in R[name]:
                m["2f" + k, e].start()

    def t4(name, e):
        for k in ("2fp", "2fm"):
            for m in R[name]:
                m[k, e].wait_recv()

    def block(l, d, j, wt):
        src = X if l == 0 else Y1
        r = ((x + d) % NX) * per_x + c * half + j
        xs = [src[bi[l * (kk // T) + k, r]] for k in range(kk // T)]
        pre = jnp.dot(jnp.concatenate(xs, axis=1), wt, preferred_element_type=jnp.float32)
        pre = pre + bias[pl.ds(l, 1), pl.ds(pl.multiple_of(r * T, T), T)]
        act = jnp.maximum(pre, 0.0).astype(jnp.bfloat16)
        if l == 0:
            Y1[r] = act
        else:
            Ob[d, :, pl.ds(pl.multiple_of(j * T, T), T)] = act
        return act.astype(jnp.float32)

    def loop(l, n, step):
        def body(t, _):
            acc[l] = step(t, acc[l])
            return 0
        lax.fori_loop(0, n, body, 0)

    def own(l, lo=0, n=half):
        def step(t, s):
            for u in range(2):
                j = lo + t * 2 + u
                s = s + block(l, 0, j, Wo[l, j])
            return s
        loop(l, n // 2, step)

    def comp_a(l, n, fa, fb):
        def step(t, s):
            a, b = fa(t), fb(t)
            s = s + block(l, 1, place(a, b), Wb[l, 0, a, b])
            return s + block(l, 3, place(b, a), Wb[l, 2, b, a])
        loop(l, n, step)

    def comp_b(l, n, fa, fb):
        def step(t, s):
            a, b = fa(t), fb(t)
            s = s + block(l, 2, place(a, b), Wb[l, 1, a, b])
            return s + block(l, 2, place(b, a), Wb[l, 1, b, a])
        loop(l, n, step)

    def comp_b_rows(l, ey):
        def step(t, s):
            for u in range(2):
                s = s + block(l, 2, place(ey, t * 2 + u), Wb[l, 1, ey, t * 2 + u])
            return s
        loop(l, 2, step)

    def diag_b(l):
        def step(t, s):
            for u in range(2):
                e = t * 2 + u
                s = s + block(l, 2, place(e, e), Wb[l, 1, e, e])
            return s
        loop(l, 2, step)

    def osl(q):
        return pl.ds(pl.multiple_of(q * half * T, half * T), half * T)

    def y1x(d, other):
        ref = Y1.at[pl.ds((((x + d) % NX) * 2 + (c + other) % 2) * half, half)]
        return rc(ref, ref, y_ss.at[d], y_rs.at[d], dev(s=1))

    def out_send(d, s, j, n=1):
        src = Ob.at[d, xrow((c + s) % 2), pl.ds(pl.multiple_of(j * T, T), n * T)]
        dst = out.at[xrow(x), pl.ds(pl.multiple_of((c * half + j) * T, T), n * T)]
        if d == 0 and s == 0:
            return pltpu.make_async_copy(src, dst, l_sem.at[3])
        return rc(src, dst, o_ss.at[d, s], o_rs.at[d, s], dev(dx=d, s=s))

    def out_wait(d, s, recv):
        if recv:
            ref = out.at[xrow((x - d + NX) % NX), osl((c + s) % 2)]
            rc(ref, ref, o_ss.at[d, s], o_rs.at[d, s], dev(dx=d, s=s)).wait_recv()
        else:
            ref = Ob.at[d, xrow((c + s) % 2), :]
            rc(ref, ref, o_ss.at[d, s], o_rs.at[d, s], dev(dx=d, s=s)).wait_send()

    def send_a(pairs):
        for a, b in pairs:
            for s in (0, 1):
                out_send(1, s, place(a, b)).start()
                out_send(3, s, place(b, a)).start()

    def send_b(pairs):
        for a, b in pairs:
            for s in (0, 1):
                out_send(2, s, place(a, b)).start()

    def start_xi(l, ds):
        for d in ds:
            xi(l, d).start()

    acc[...] = jnp.zeros_like(acc)
    local[2].wait()
    start_xi(0, (1, 3))
    pltpu.make_async_copy(im, im, im_sem).wait()
    xa_send(1).start()
    xa_send(3).start()
    start_xi(0, (2,))
    xa_send(2).start()
    xf(0).start()
    mine_x = pltpu.make_async_copy(im.at[:, xrow(x), :], X.at[xblk(x), xrow(c), :], l_sem.at[5])
    mine_x.start()
    for cp in (local[0], local[1], local[3], mine_x):
        cp.wait()
    start_xi(1, (2, 1, 3))
    for k in range(len(FAR)):
        for h in (0, 1):
            far(h, k).start()

    t0("a0")
    t1("a0")
    t3("a0", 0)
    t0("b0")
    t2("a0")
    t3("a0", 3)
    t3("a0", 1)
    t1("b0")
    t3("a0", 2)
    t3("b0", 0)
    t2("b0")
    for d in (1, 3, 2):
        xa_recv(d).wait_recv()
        xf(d).start()
    t3("b0", 3)
    for d in (0, 1, 3, 2):
        xf(d, other=1).wait_recv()
    own(0)
    y1x(0, 0).start()
    t0("b1")
    t3("b0", 1)
    for e in range(4):
        t4("a0", e)
    comp_a(0, 4, lambda t: 0, lambda t: t)
    t3("b0", 2)
    comp_a(0, 4, lambda t: 1, lambda t: t)
    t1("b1")
    comp_a(0, 8, lambda t: 2 + t // 4, lambda t: t % 4)
    y1x(1, 0).start()
    y1x(3, 0).start()
    for e in range(4):
        t4("b0", e)
    for ey in range(4):
        comp_b_rows(0, ey)
    y1x(2, 0).start()
    t3("b1", 0)
    t2("b1")
    t0("a1")
    t3("b1", 3)
    t3("b1", 1)
    for h in (0, 1):
        far(h, 0).wait_recv()
        for k in ("2p", "2m"):
            R["a1"][h][k, 2].start()
    for d in range(4):
        y1x(d, 1).wait_recv()
    comp_b(1, 1, lambda t: 0, lambda t: 1)
    comp_b(1, 1, lambda t: 0, lambda t: 3)
    send_b([(0, 1), (1, 0), (0, 3), (3, 0)])
    t3("b1", 2)
    comp_b(1, 1, lambda t: 1, lambda t: 3)
    send_b([(1, 3), (3, 1)])
    for k in range(1, len(FAR)):
        for h in (0, 1):
            far(h, k).wait_recv()
    comp_a(1, 2, lambda t: 2 * t, lambda t: 0)
    send_a([(0, 0), (2, 0)])
    comp_a(1, 4, lambda t: t, lambda t: 2)
    send_a([(0, 2), (1, 2), (2, 2), (3, 2)])
    for k in "pm":
        for m in R["a1"]:
            m["1" + k].wait_recv()
    for e in (3, 1):
        for k in ("2p", "2m"):
            for m in R["a1"]:
                m[k, e].start()
    for e in (0, 3, 1, 2):
        t4("b1", e)
    comp_b(1, 1, lambda t: 0, lambda t: 2)
    comp_b(1, 2, lambda t: 1 + 2 * t, lambda t: 2)
    diag_b(1)
    send_b([(0, 2), (2, 0), (0, 0), (1, 1), (2, 2), (3, 3), (1, 2), (2, 1), (3, 2), (2, 3)])
    comp_a(1, 2, lambda t: 1 + 2 * t, lambda t: 0)
    send_a([(1, 0), (3, 0)])
    own(1)
    for s in (0, 1):
        out_send(0, s, 0, half).start()
    for e, ce in ((0, lambda t: 0), (2, lambda t: 2), (3, lambda t: 3), (1, lambda t: 1)):
        for k in "pm":
            for m in R["a1"]:
                m["2" + k, e].wait_recv()
        comp_a(1, 2, ce, lambda t: 1 + 2 * t)
        send_a([(e, 1), (e, 3)])

    ax = rc(acc.at[:, xrow((c + 1) % 2), :], accr, a_ss.at[0], a_rs.at[0], dev(s=1))
    ax.start()
    mine = acc[:, xrow(c), :]
    ax.wait_recv()
    tot = jnp.sum(mine + accr[...], axis=2)
    share = jnp.minimum(1.0, tot * (1.0 / (NX * cols * LIVE_LEVEL)))
    part_sum = jnp.broadcast_to(jnp.sum(share, axis=1, keepdims=True), (2, T))

    def gather_sum(buf, n, me, val, targets, base):
        buf[me] = val
        cps = [rc(buf.at[me], buf.at[me], z_ss.at[base + k], z_rs.at[base + k], t) for k, (t, _) in enumerate(targets)]
        for cp in cps:
            cp.start()
        for k, (_, who) in enumerate(targets):
            rc(buf.at[who], buf.at[who], z_ss.at[base + k], z_rs.at[base + k], dev(s=1)).wait_recv()
        total = buf[0]
        for k in range(1, n):
            total = total + buf[k]
        return total, cps

    far_first = sorted(range(1, NZ), key=lambda d: -min(d, NZ - d))
    v, cz = gather_sum(rz, NZ, z, part_sum, [(dev(dz=d), (z - d + NZ) % NZ) for d in far_first], 0)
    v, cy = gather_sum(ry, NY, y, v, [(dev(dy=d), (y - d + NY) % NY) for d in (2, 1, 3)], NZ)
    me_x = [(dev(dx=d, s=s), ((x - d + NX) % NX) * 2 + (c + s) % 2) for d in (2, 1, 3, 0) for s in (0, 1) if d or s]
    v, cx = gather_sum(rx, 2 * NX, x * 2 + c, v, me_x, NZ + NY)
    v = v * (1.0 / (NX * rows * 2 * NZ * NY))
    for l in range(2):
        stat[l] = jnp.sum(v[l:l + 1, 0:1])

    for cp in cz + cy + cx:
        cp.wait_send()
    for l in range(2):
        for d in (1, 2, 3):
            xi(l, d).wait_send()
    for h in (0, 1):
        for k in range(len(FAR)):
            far(h, k).wait_send()
    for name in RINGS:
        for m in R[name]:
            for cp in m["sends"]:
                cp.wait_send()
    for d in (1, 2, 3):
        xa_send(d).wait_send()
    for d in range(4):
        xf(d).wait_send()
        y1x(d, 0).wait_send()
    ax.wait_send()
    out_send(0, 0, 0, half).wait()
    for d in range(4):
        for s in (0, 1):
            if d or s:
                out_wait(d, s, True)
                out_wait(d, s, False)


def per_device(images, weights, block_index, bias):
    n_img, cols = images.shape
    layers, per_x, kk, _ = weights.shape
    rows = n_img // NX
    half = per_x // 2
    total = cols * NX
    dma = pltpu.SemaphoreType.DMA
    any_ = pl.BlockSpec(memory_space=pl.ANY)
    index = jnp.transpose(block_index, (0, 2, 1)).reshape(layers * (kk // T), total // T)
    return pl.pallas_call(
        kernel,
        out_shape=(jax.ShapeDtypeStruct((n_img, cols), jnp.bfloat16), jax.ShapeDtypeStruct((layers,), jnp.float32)),
        in_specs=[any_] * 4,
        out_specs=(any_, pl.BlockSpec(memory_space=pltpu.SMEM)),
        scratch_shapes=[
            pltpu.VMEM((per_x, n_img, T), jnp.bfloat16),
            pltpu.VMEM((total // T, 2 * rows, T), jnp.bfloat16),
            pltpu.VMEM((total // T, 2 * rows, T), jnp.bfloat16),
            pltpu.VMEM((layers, 3, NY, NW, kk, T), jnp.bfloat16),
            pltpu.VMEM((layers, half, kk, T), jnp.bfloat16),
            pltpu.VMEM((NX, 2 * rows, half * T), jnp.bfloat16),
            pltpu.VMEM((layers, 2 * rows, T), jnp.float32),
            pltpu.VMEM((layers, rows, T), jnp.float32),
            pltpu.VMEM((NZ, layers, T), jnp.float32),
            pltpu.VMEM((NY, layers, T), jnp.float32),
            pltpu.VMEM((2 * NX, layers, T), jnp.float32),
            pltpu.SMEM(index.shape, jnp.int32),
            pltpu.VMEM(bias.shape, jnp.float32),
            dma((8,)), dma((8,)),
            dma((layers, 3)), dma((layers, 3)),
            dma((2, 5)), dma((2, 5)),
            dma((4, 2, 8)), dma((4, 2, 20)),
            dma((4,)), dma((4,)),
            dma((4, 2)), dma((4, 2)),
            dma((1,)), dma((1,)),
            dma((6,)), dma,
            dma((20,)), dma((20,)),
        ],
        compiler_params=pltpu.CompilerParams(collective_id=0, has_side_effects=True, vmem_limit_bytes=60 * 1024 * 1024),
        name="sparse_net",
    )(images, weights, index, bias)


def solution(mesh):
    return jax.shard_map(
        per_device, mesh=mesh,
        in_specs=(P("img", "nrn"), P(None, "nrn", None, None), P(), P()),
        out_specs=(P("img", "nrn"), P()), check_vma=False,
    )
```

```python
import jax
import jax.numpy as jnp
from jax import lax
from jax.experimental import pallas as pl
from jax.experimental.pallas import tpu as pltpu
from jax.sharding import PartitionSpec as P

MESH = pl.DeviceIdType.MESH
LIVE_LEVEL = 0.25
NX, NY, NZ, NW = 4, 4, 8, 4
T = 128


A1_SENDS = 3
RINGS = {"a0": 0, "b0": 1, "b1": 2, "a1": 3}


def kernel(img, w, bi_hbm, bias_hbm, out, stat, im, X, Y1, Wb, Wo, Ob, acc, accr, rz, ry, rx, bi, bias, Wx,
           x_ss, x_rs, xi_ss, xi_rs, xp_rs, x2_ss, x2_rs, far_ss, far_rs, w_ss, w_rs, y_ss, y_rs, o_ss, o_rs, a_ss, a_rs, l_sem, im_sem, wx_sem, z_ss, z_rs):
    x = lax.axis_index("nrn")
    i = lax.axis_index("img")
    c = i % 2
    z = (i // 2) % NZ
    y = i // (2 * NZ)
    zm = z % NW
    rows = img.shape[0] // NX
    cols = img.shape[1]
    per_x = w.shape[1]
    half = per_x // 2
    kk = w.shape[2]

    def dev(dx=0, dy=0, dz=0, s=0):
        cc = (c + s) % 2
        return (((y + dy + NY) % NY) * 2 * NZ + ((z + dz + NZ) % NZ) * 2 + cc, (x + dx + NX) % NX)

    def rc(src, dst, ss, rs, d):
        return pltpu.make_async_remote_copy(src_ref=src, dst_ref=dst, send_sem=ss, recv_sem=rs,
                                            device_id=d, device_id_type=MESH)

    partners = [dev(dx=d, s=s) for d in (2, 1, 3) for s in (0, 1)]
    partners += [dev(dz=1), dev(dz=-1), dev(dy=1), dev(dy=-1), dev(s=1)]
    bar = pltpu.get_barrier_semaphore()
    for p in partners:
        pl.semaphore_signal(bar, 1, device_id=p, device_id_type=MESH)
    imc = [pltpu.make_async_copy(img.at[:, pl.ds(b * T, T)], im.at[b], im_sem) for b in range(per_x)]
    local = [pltpu.make_async_copy(bi_hbm, bi, l_sem.at[2]), pltpu.make_async_copy(bias_hbm, bias, l_sem.at[4])]
    local += [pltpu.make_async_copy(w.at[l, pl.ds(pl.multiple_of(c * half, half), half)], Wo.at[l], l_sem.at[l])
              for l in range(2)]
    first = [pltpu.make_async_copy(w.at[l, c * half + y * NW + zm], Wx.at[l], wx_sem.at[l]) for l in range(2)]
    for cp in first + imc + local[2:3] + local[:2] + local[3:]:
        cp.start()
    pl.semaphore_wait(bar, len(partners))

    def xrow(g):
        return pl.ds(pl.multiple_of(g * rows, rows), rows)

    def xblk(q):
        return pl.ds(q * per_x, per_x)

    def xa_send(d):
        t = (x + d) % NX
        return rc(im.at[:, xrow(t), :], X.at[xblk(x), xrow(c), :], x_ss.at[d], x_rs.at[d], dev(dx=d))

    def xa_recv(d):
        q = (x - d + NX) % NX
        return rc(im.at[:, xrow(x), :], X.at[xblk(q), xrow(c), :], x_ss.at[d], x_rs.at[d], dev(dx=d))

    def xf(d, other=0):
        q = (x - d + NX) % NX
        ref = X.at[xblk(q), xrow((c + other) % 2), :]
        src = im.at[:, xrow(x), :] if d == 0 and not other else ref
        k = 4 + d
        return rc(src, ref, x_ss.at[k], x_rs.at[k], dev(s=1))

    j0 = y * NW + zm

    def place(ey, ez):
        return ((y + ey) % NY) * NW + (zm + ez) % NW

    def xi(l, d):
        return rc(Wx.at[l], Wb.at[l, d - 1, 0, 0], xi_ss.at[l, d - 1], xi_rs.at[l, d - 1], dev(dx=-d))

    def xi_part(d, p):
        r = pl.ds(p * (kk // 2), kk // 2)
        return rc(Wx.at[0, r, :], Wb.at[0, d - 1, 0, 0, r, :], xi_ss.at[0, d - 1], xp_rs.at[d // 2, p], dev(dx=-d))

    def xi2(l, h):
        d = (1, 3)[h]
        r = pl.ds(h * (kk // 2), kk // 2)
        return rc(Wb.at[l, d - 1, 0, 0, r, :], Wb.at[l, 1, 0, 0, r, :], x2_ss.at[l, h], x2_rs.at[l, h], dev(dx=-d))

    FAR = ((0, 2), (2, 2), (1, 2), (3, 2), (2, 0), (2, 1), (2, 3))

    NF = len(FAR)

    def far(h, k):
        a, b = FAR[k]
        d = (1, 3)[h]
        ey, ez = (b, a) if h else (a, b)
        return rc(Wo.at[1, place(ey, ez)], Wb.at[1, d - 1, ey, ez], far_ss.at[h, k], far_rs.at[h, k], dev(dx=-d))

    def ring(name):
        n, l = RINGS[name], int(name[1])
        halves = []
        for h in (0, 1):
            if name[0] == "a":
                d, lo, size = (1, 3)[h], 0, kk
            else:
                d, lo, size = 2, h * (kk // 2), kk // 2
            q = size // 2

            def slot(a, b, off, m, d=d, h=h, lo=lo):
                ey, ez = (b, a) if h else (a, b)
                return Wb.at[l, d - 1, ey, ez, pl.ds(lo + off, m), :]

            up1, dn1, up2, dn2 = dev(dy=1), dev(dy=-1), dev(dz=1), dev(dz=-1)
            if h:
                up1, dn1, up2, dn2 = up2, dn2, up1, dn1
            ss, rs = w_ss.at[n, h], w_rs.at[n, h]
            m = {}
            m["1p"] = rc(slot(0, 0, 0, size), slot(3, 0, 0, size), ss.at[0], rs.at[0], up1)
            m["1m"] = rc(slot(0, 0, 0, size), slot(1, 0, 0, size), ss.at[1], rs.at[1], dn1)
            m["1fp"] = rc(slot(3, 0, 0, q), slot(2, 0, 0, q), ss.at[2], rs.at[2], up1)
            m["1fm"] = rc(slot(1, 0, q, q), slot(2, 0, q, q), ss.at[3], rs.at[3], dn1)
            for e in range(4):
                m["2p", e] = rc(slot(e, 0, 0, size), slot(e, 3, 0, size), ss.at[4], rs.at[4 + e], up2)
                m["2m", e] = rc(slot(e, 0, 0, size), slot(e, 1, 0, size), ss.at[5], rs.at[8 + e], dn2)
                m["2fp", e] = rc(slot(e, 3, 0, q), slot(e, 2, 0, q), ss.at[6], rs.at[12 + e], up2)
                m["2fm", e] = rc(slot(e, 1, q, q), slot(e, 2, q, q), ss.at[7], rs.at[16 + e], dn2)
            sends = [m["1p"], m["1m"], m["1fp"], m["1fm"]]
            for k, b, off, size_k in ((4, 0, 0, size), (5, 0, 0, size), (6, 3, 0, q), (7, 1, q, q)):
                r = slot(slice(0, A1_SENDS if name == "a1" else 4), b, off, size_k)
                sends.append(rc(r, r, ss.at[k], rs.at[4], up2))
            m["start"] = []
            for p in (0, 1):
                o, n_ = p * q, q
                m["start"].append([
                    rc(slot(0, 0, o, n_), slot(3, 0, o, n_), ss.at[0], rs.at[0], up1),
                    rc(slot(0, 0, o, n_), slot(1, 0, o, n_), ss.at[1], rs.at[1], dn1),
                    rc(slot(0, 0, o, n_), slot(0, 3, o, n_), ss.at[4], rs.at[4], up2),
                    rc(slot(0, 0, o, n_), slot(0, 1, o, n_), ss.at[5], rs.at[8], dn2)])
            m["sends"] = sends[:2] + sends[4:6] if name == "a1" else sends
            halves.append(m)
        return halves

    R = {name: ring(name) for name in RINGS}

    def t0(name):
        l = int(name[1])
        if name == "a0":
            for p in (0, 1):
                for d in (1, 3):
                    xi_part(d, p).wait_recv()
                for k in range(4):
                    for m in R[name]:
                        m["start"][p][k].start()
            return
        if name[0] == "b":
            for h in (0, 1):
                xi2(l, h).wait_recv()
        for k in ("1p", "1m", ("2p", 0), ("2m", 0)):
            for m in R[name]:
                m[k].start()

    def t1(name):
        for k in "pm":
            for m in R[name]:
                m["1" + k].wait_recv()
            for m in R[name]:
                m["1f" + k].start()
        for e in (3, 1):
            for k in ("2p", "2m"):
                for m in R[name]:
                    m[k, e].start()

    def t2(name):
        for k in ("1fp", "1fm"):
            for m in R[name]:
                m[k].wait_recv()
        for k in ("2p", "2m"):
            for m in R[name]:
                m[k, 2].start()

    def t3(name, e):
        for k in "pm":
            for m in R[name]:
                m["2" + k, e].wait_recv()
            for m in R[name]:
                m["2f" + k, e].start()

    def t4(name, e):
        for k in ("2fp", "2fm"):
            for m in R[name]:
                m[k, e].wait_recv()

    def block(l, d, j, wt):
        src = X if l == 0 else Y1
        r = ((x + d) % NX) * per_x + c * half + j
        xs = [src[bi[l * (kk // T) + k, r]] for k in range(kk // T)]
        pre = jnp.dot(jnp.concatenate(xs, axis=1), wt, preferred_element_type=jnp.float32)
        pre = pre + bias[pl.ds(l, 1), pl.ds(pl.multiple_of(r * T, T), T)]
        act = jnp.maximum(pre, 0.0).astype(jnp.bfloat16)
        if l == 0:
            Y1[r] = act
        else:
            Ob[d, :, pl.ds(pl.multiple_of(j * T, T), T)] = act
        return act.astype(jnp.float32)

    def loop(l, n, step):
        def body(t, _):
            acc[l] = step(t, acc[l])
            return 0
        lax.fori_loop(0, n, body, 0)

    def own(l, lo=0, n=half):
        def step(t, s):
            for u in range(2):
                j = lo + t * 2 + u
                s = s + block(l, 0, j, Wo[l, j])
            return s
        loop(l, n // 2, step)

    def comp_a(l, n, fa, fb):
        def step(t, s):
            a, b = fa(t), fb(t)
            s = s + block(l, 1, place(a, b), Wb[l, 0, a, b])
            return s + block(l, 3, place(b, a), Wb[l, 2, b, a])
        loop(l, n, step)

    def comp_b(l, n, fa, fb):
        def step(t, s):
            a, b = fa(t), fb(t)
            s = s + block(l, 2, place(a, b), Wb[l, 1, a, b])
            return s + block(l, 2, place(b, a), Wb[l, 1, b, a])
        loop(l, n, step)

    def comp_b_rows(l, ey):
        def step(t, s):
            for u in range(2):
                s = s + block(l, 2, place(ey, t * 2 + u), Wb[l, 1, ey, t * 2 + u])
            return s
        loop(l, 2, step)

    def diag_b(l):
        def step(t, s):
            for u in range(2):
                e = t * 2 + u
                s = s + block(l, 2, place(e, e), Wb[l, 1, e, e])
            return s
        loop(l, 2, step)

    def osl(q):
        return pl.ds(pl.multiple_of(q * half * T, half * T), half * T)

    def y1x(d, other):
        ref = Y1.at[pl.ds((((x + d) % NX) * 2 + (c + other) % 2) * half, half)]
        return rc(ref, ref, y_ss.at[d], y_rs.at[d], dev(s=1))

    def out_send(d, s, j, n=1):
        src = Ob.at[d, xrow((c + s) % 2), pl.ds(pl.multiple_of(j * T, T), n * T)]
        dst = out.at[xrow(x), pl.ds(pl.multiple_of((c * half + j) * T, T), n * T)]
        if d == 0 and s == 0:
            return pltpu.make_async_copy(src, dst, l_sem.at[3])
        return rc(src, dst, o_ss.at[d, s], o_rs.at[d, s], dev(dx=d, s=s))

    def out_wait(d, s, recv):
        if recv:
            ref = out.at[xrow((x - d + NX) % NX), osl((c + s) % 2)]
            rc(ref, ref, o_ss.at[d, s], o_rs.at[d, s], dev(dx=d, s=s)).wait_recv()
        else:
            ref = Ob.at[d, xrow((c + s) % 2), :]
            rc(ref, ref, o_ss.at[d, s], o_rs.at[d, s], dev(dx=d, s=s)).wait_send()

    def send_a(pairs):
        for a, b in pairs:
            for s in (0, 1):
                out_send(1, s, place(a, b)).start()
                out_send(3, s, place(b, a)).start()

    def send_b(pairs):
        for a, b in pairs:
            for s in (0, 1):
                out_send(2, s, place(a, b)).start()

    def start_xi(l, ds):
        for d in ds:
            xi(l, d).start()

    acc[...] = jnp.zeros_like(acc)
    first[0].wait()
    for p in (0, 1):
        for d in (1, 3):
            xi_part(d, p).start()
    first[1].wait()
    start_xi(1, (1, 3))
    pltpu.make_async_copy(im, im, im_sem).wait()
    xf(0).start()
    mine_x = pltpu.make_async_copy(im.at[:, xrow(x), :], X.at[xblk(x), xrow(c), :], l_sem.at[5])
    mine_x.start()
    local.append(mine_x)

    t0("a0")
    for h in (0, 1):
        xi2(0, h).start()
    for d in (1, 3, 2):
        xa_send(d).start()
    t1("a0")
    for d in (1, 3):
        xi(1, d).wait_recv()
    for h in (0, 1):
        xi2(1, h).start()
    for cp in local:
        cp.wait()
    for k in range(NF):
        for h in (0, 1):
            far(h, k).start()
    t3("a0", 0)
    t0("b0")
    t2("a0")
    t3("a0", 3)
    t3("a0", 1)
    t1("b0")
    t3("a0", 2)
    t3("b0", 0)
    t2("b0")
    for d in (1, 3, 2):
        xa_recv(d).wait_recv()
        xf(d).start()
    t3("b0", 3)
    for d in (0, 1, 3, 2):
        xf(d, other=1).wait_recv()
    own(0)
    y1x(0, 0).start()
    t0("b1")
    t3("b0", 1)
    for e in range(4):
        t4("a0", e)
    comp_a(0, 4, lambda t: 0, lambda t: t)
    t3("b0", 2)
    comp_a(0, 4, lambda t: 1, lambda t: t)
    t1("b1")
    comp_a(0, 8, lambda t: 2 + t // 4, lambda t: t % 4)
    y1x(1, 0).start()
    y1x(3, 0).start()
    for e in range(4):
        t4("b0", e)
    for ey in range(4):
        comp_b_rows(0, ey)
    y1x(2, 0).start()
    t3("b1", 0)
    t2("b1")
    t0("a1")
    t3("b1", 3)
    t3("b1", 1)
    for d in range(4):
        y1x(d, 1).wait_recv()
    comp_b(1, 1, lambda t: 0, lambda t: 1)
    comp_b(1, 1, lambda t: 0, lambda t: 3)
    send_b([(0, 1), (1, 0), (0, 3), (3, 0)])
    t3("b1", 2)
    comp_b(1, 1, lambda t: 1, lambda t: 3)
    send_b([(1, 3), (3, 1)])
    for k in range(NF):
        for h in (0, 1):
            far(h, k).wait_recv()
    comp_a(1, 2, lambda t: 2 * t, lambda t: 0)
    send_a([(0, 0), (2, 0)])
    comp_a(1, 4, lambda t: t, lambda t: 2)
    comp_a(1, 2, lambda t: 2, lambda t: 1 + 2 * t)
    send_a([(0, 2), (1, 2), (2, 2), (3, 2), (2, 1), (2, 3)])
    for k in "pm":
        for m in R["a1"]:
            m["1" + k].wait_recv()
    for e in (3, 1):
        for k in ("2p", "2m"):
            for m in R["a1"]:
                m[k, e].start()
    for e in (0, 3, 1, 2):
        t4("b1", e)
    comp_b(1, 1, lambda t: 0, lambda t: 2)
    comp_b(1, 2, lambda t: 1 + 2 * t, lambda t: 2)
    diag_b(1)
    send_b([(0, 2), (2, 0), (0, 0), (1, 1), (2, 2), (3, 3), (1, 2), (2, 1), (3, 2), (2, 3)])
    comp_a(1, 2, lambda t: 1 + 2 * t, lambda t: 0)
    send_a([(1, 0), (3, 0)])
    own(1)
    for s in (0, 1):
        out_send(0, s, 0, half).start()
    for e, ce in ((0, lambda t: 0), (3, lambda t: 3), (1, lambda t: 1)):
        for k in "pm":
            for m in R["a1"]:
                m["2" + k, e].wait_recv()
        comp_a(1, 2, ce, lambda t: 1 + 2 * t)
        send_a([(e, 1), (e, 3)])

    ax = rc(acc.at[:, xrow((c + 1) % 2), :], accr, a_ss.at[0], a_rs.at[0], dev(s=1))
    ax.start()
    mine = acc[:, xrow(c), :]
    ax.wait_recv()
    tot = jnp.sum(mine + accr[...], axis=2)
    share = jnp.minimum(1.0, tot * (1.0 / (NX * cols * LIVE_LEVEL)))
    part_sum = jnp.broadcast_to(jnp.sum(share, axis=1, keepdims=True), (2, T))

    def gather_sum(buf, n, me, val, targets, base):
        buf[me] = val
        cps = [rc(buf.at[me], buf.at[me], z_ss.at[base + k], z_rs.at[base + k], t) for k, (t, _) in enumerate(targets)]
        for cp in cps:
            cp.start()
        for k, (_, who) in enumerate(targets):
            rc(buf.at[who], buf.at[who], z_ss.at[base + k], z_rs.at[base + k], dev(s=1)).wait_recv()
        total = buf[0]
        for k in range(1, n):
            total = total + buf[k]
        return total, cps

    far_first = sorted(range(1, NZ), key=lambda d: -min(d, NZ - d))
    v, cz = gather_sum(rz, NZ, z, part_sum, [(dev(dz=d), (z - d + NZ) % NZ) for d in far_first], 0)
    v, cy = gather_sum(ry, NY, y, v, [(dev(dy=d), (y - d + NY) % NY) for d in (2, 1, 3)], NZ)
    me_x = [(dev(dx=d, s=s), ((x - d + NX) % NX) * 2 + (c + s) % 2) for d in (2, 1, 3, 0) for s in (0, 1) if d or s]
    v, cx = gather_sum(rx, 2 * NX, x * 2 + c, v, me_x, NZ + NY)
    v = v * (1.0 / (NX * rows * 2 * NZ * NY))
    for l in range(2):
        stat[l] = jnp.sum(v[l:l + 1, 0:1])

    for cp in cz + cy + cx:
        cp.wait_send()
    for l in range(2):
        for d in (1, 3):
            xi(l, d).wait_send()
        for h in (0, 1):
            xi2(l, h).wait_send()
    for h in (0, 1):
        for k in range(len(FAR)):
            far(h, k).wait_send()
    for name in RINGS:
        for m in R[name]:
            for cp in m["sends"]:
                cp.wait_send()
    for d in (1, 2, 3):
        xa_send(d).wait_send()
    for d in range(4):
        xf(d).wait_send()
        y1x(d, 0).wait_send()
    ax.wait_send()
    out_send(0, 0, 0, half).wait()
    for d in range(4):
        for s in (0, 1):
            if d or s:
                out_wait(d, s, True)
                out_wait(d, s, False)


def per_device(images, weights, block_index, bias):
    n_img, cols = images.shape
    layers, per_x, kk, _ = weights.shape
    rows = n_img // NX
    half = per_x // 2
    total = cols * NX
    dma = pltpu.SemaphoreType.DMA
    any_ = pl.BlockSpec(memory_space=pl.ANY)
    index = jnp.transpose(block_index, (0, 2, 1)).reshape(layers * (kk // T), total // T)
    return pl.pallas_call(
        kernel,
        out_shape=(jax.ShapeDtypeStruct((n_img, cols), jnp.bfloat16), jax.ShapeDtypeStruct((layers,), jnp.float32)),
        in_specs=[any_] * 4,
        out_specs=(any_, pl.BlockSpec(memory_space=pltpu.SMEM)),
        scratch_shapes=[
            pltpu.VMEM((per_x, n_img, T), jnp.bfloat16),
            pltpu.VMEM((total // T, 2 * rows, T), jnp.bfloat16),
            pltpu.VMEM((total // T, 2 * rows, T), jnp.bfloat16),
            pltpu.VMEM((layers, 3, NY, NW, kk, T), jnp.bfloat16),
            pltpu.VMEM((layers, half, kk, T), jnp.bfloat16),
            pltpu.VMEM((NX, 2 * rows, half * T), jnp.bfloat16),
            pltpu.VMEM((layers, 2 * rows, T), jnp.float32),
            pltpu.VMEM((layers, rows, T), jnp.float32),
            pltpu.VMEM((NZ, layers, T), jnp.float32),
            pltpu.VMEM((NY, layers, T), jnp.float32),
            pltpu.VMEM((2 * NX, layers, T), jnp.float32),
            pltpu.SMEM(index.shape, jnp.int32),
            pltpu.VMEM(bias.shape, jnp.float32),
            pltpu.VMEM((layers, kk, T), jnp.bfloat16),
            dma((8,)), dma((8,)),
            dma((layers, 3)), dma((layers, 3)), dma((2, 2)), dma((layers, 2)), dma((layers, 2)),
            dma((2, 7)), dma((2, 7)),
            dma((4, 2, 8)), dma((4, 2, 20)),
            dma((4,)), dma((4,)),
            dma((4, 2)), dma((4, 2)),
            dma((1,)), dma((1,)),
            dma((6,)), dma, dma((2,)),
            dma((20,)), dma((20,)),
        ],
        compiler_params=pltpu.CompilerParams(collective_id=0, has_side_effects=True, vmem_limit_bytes=50 * 1024 * 1024),
        name="sparse_net",
    )(images, weights, index, bias)


def solution(mesh):
    return jax.shard_map(
        per_device, mesh=mesh,
        in_specs=(P("img", "nrn"), P(None, "nrn", None, None), P(), P()),
        out_specs=(P("img", "nrn"), P()), check_vma=False,
    )
```

```python
import jax
import jax.numpy as jnp
from jax import lax
from jax.experimental import pallas as pl
from jax.experimental.pallas import tpu as pltpu
from jax.sharding import PartitionSpec as P

MESH = pl.DeviceIdType.MESH
LIVE_LEVEL = 0.25
NX, NY, NZ, NW = 4, 4, 8, 4
T = 128


A1_SENDS = 3
RINGS = {"a0": 0, "b0": 1, "b1": 2, "a1": 3}


def kernel(img, w, bi_hbm, bias_hbm, out, stat, im, X, Y1, Wb, Wo, Ob, acc, accr, rz, rx, bi, bias, Wx,
           x_ss, x_rs, xi_ss, xi_rs, xp_rs, x2_ss, x2_rs, far_ss, far_rs, w_ss, w_rs, y_ss, y_rs, o_ss, o_rs, a_ss, a_rs, l_sem, im_sem, wx_sem, z_ss, z_rs):
    x = lax.axis_index("nrn")
    i = lax.axis_index("img")
    c = i % 2
    z = (i // 2) % NZ
    y = i // (2 * NZ)
    zm = z % NW
    rows = img.shape[0] // NX
    cols = img.shape[1]
    per_x = w.shape[1]
    half = per_x // 2
    kk = w.shape[2]

    def dev(dx=0, dy=0, dz=0, s=0):
        cc = (c + s) % 2
        return (((y + dy + NY) % NY) * 2 * NZ + ((z + dz + NZ) % NZ) * 2 + cc, (x + dx + NX) % NX)

    def rc(src, dst, ss, rs, d):
        return pltpu.make_async_remote_copy(src_ref=src, dst_ref=dst, send_sem=ss, recv_sem=rs,
                                            device_id=d, device_id_type=MESH)

    partners = [dev(dx=d, s=s) for d in (2, 1, 3) for s in (0, 1)]
    partners += [dev(dz=1), dev(dz=-1), dev(dy=1), dev(dy=-1), dev(s=1)]
    bar = pltpu.get_barrier_semaphore()
    for p in partners:
        pl.semaphore_signal(bar, 1, device_id=p, device_id_type=MESH)
    imc = [pltpu.make_async_copy(img.at[:, pl.ds(b * T, T)], im.at[b], im_sem) for b in range(per_x)]
    local = [pltpu.make_async_copy(bi_hbm, bi, l_sem.at[2]), pltpu.make_async_copy(bias_hbm, bias, l_sem.at[4])]
    local += [pltpu.make_async_copy(w.at[l, pl.ds(pl.multiple_of(c * half, half), half)], Wo.at[l], l_sem.at[l])
              for l in range(2)]
    first = [pltpu.make_async_copy(w.at[l, c * half + y * NW + zm], Wx.at[l], wx_sem.at[l]) for l in range(2)]
    for cp in first + imc + local[2:3] + local[:2] + local[3:]:
        cp.start()
    pl.semaphore_wait(bar, len(partners))

    def xrow(g):
        return pl.ds(pl.multiple_of(g * rows, rows), rows)

    def xblk(q):
        return pl.ds(q * per_x, per_x)

    def xa_send(d):
        t = (x + d) % NX
        return rc(im.at[:, xrow(t), :], X.at[xblk(x), xrow(c), :], x_ss.at[d], x_rs.at[d], dev(dx=d))

    def xa_recv(d):
        q = (x - d + NX) % NX
        return rc(im.at[:, xrow(x), :], X.at[xblk(q), xrow(c), :], x_ss.at[d], x_rs.at[d], dev(dx=d))

    def xf(d, other=0):
        q = (x - d + NX) % NX
        ref = X.at[xblk(q), xrow((c + other) % 2), :]
        src = im.at[:, xrow(x), :] if d == 0 and not other else ref
        k = 4 + d
        return rc(src, ref, x_ss.at[k], x_rs.at[k], dev(s=1))

    j0 = y * NW + zm

    def place(ey, ez):
        return ((y + ey) % NY) * NW + (zm + ez) % NW

    def xi(l, d):
        return rc(Wx.at[l], Wb.at[l, d - 1, 0, 0], xi_ss.at[l, d - 1], xi_rs.at[l, d - 1], dev(dx=-d))

    def xi_part(d, p):
        r = pl.ds(p * (kk // 2), kk // 2)
        return rc(Wx.at[0, r, :], Wb.at[0, d - 1, 0, 0, r, :], xi_ss.at[0, d - 1], xp_rs.at[d // 2, p], dev(dx=-d))

    def xi2(l, h):
        d = (1, 3)[h]
        r = pl.ds(h * (kk // 2), kk // 2)
        return rc(Wb.at[l, d - 1, 0, 0, r, :], Wb.at[l, 1, 0, 0, r, :], x2_ss.at[l, h], x2_rs.at[l, h], dev(dx=-d))

    FAR = ((0, 2), (2, 2), (1, 2), (3, 2), (2, 0), (2, 3), (2, 1))

    NF = len(FAR)

    def far(h, k):
        a, b = FAR[k]
        d = (1, 3)[h]
        ey, ez = (b, a) if h else (a, b)
        r = pl.ds(0, kk) if k < 5 else pl.ds((k - 5) * (kk // 2), kk // 2)
        return rc(Wo.at[1, place(ey, ez), r, :], Wb.at[1, d - 1, ey, ez, r, :], far_ss.at[h, k], far_rs.at[h, k], dev(dx=-d))

    def ring(name):
        n, l = RINGS[name], int(name[1])
        halves = []
        for h in (0, 1):
            if name[0] == "a":
                d, lo, size = (1, 3)[h], 0, kk
            else:
                d, lo, size = 2, h * (kk // 2), kk // 2
            q = size // 2

            def slot(a, b, off, m, d=d, h=h, lo=lo):
                ey, ez = (b, a) if h else (a, b)
                return Wb.at[l, d - 1, ey, ez, pl.ds(lo + off, m), :]

            up1, dn1, up2, dn2 = dev(dy=1), dev(dy=-1), dev(dz=1), dev(dz=-1)
            if h:
                up1, dn1, up2, dn2 = up2, dn2, up1, dn1
            ss, rs = w_ss.at[n, h], w_rs.at[n, h]
            m = {}
            m["1p"] = rc(slot(0, 0, 0, size), slot(3, 0, 0, size), ss.at[0], rs.at[0], up1)
            m["1m"] = rc(slot(0, 0, 0, size), slot(1, 0, 0, size), ss.at[1], rs.at[1], dn1)
            m["1fp"] = rc(slot(3, 0, 0, q), slot(2, 0, 0, q), ss.at[2], rs.at[2], up1)
            m["1fm"] = rc(slot(1, 0, q, q), slot(2, 0, q, q), ss.at[3], rs.at[3], dn1)
            for e in range(4):
                m["2p", e] = rc(slot(e, 0, 0, size), slot(e, 3, 0, size), ss.at[4], rs.at[4 + e], up2)
                m["2m", e] = rc(slot(e, 0, 0, size), slot(e, 1, 0, size), ss.at[5], rs.at[8 + e], dn2)
                m["2fp", e] = rc(slot(e, 3, 0, q), slot(e, 2, 0, q), ss.at[6], rs.at[12 + e], up2)
                m["2fm", e] = rc(slot(e, 1, q, q), slot(e, 2, q, q), ss.at[7], rs.at[16 + e], dn2)
            m["hp"] = rc(slot(2, 0, q, q), slot(2, 3, q, q), ss.at[6], rs.at[6], up2)
            m["hm"] = rc(slot(2, 0, 0, q), slot(2, 1, 0, q), ss.at[7], rs.at[10], dn2)
            sends = [m["1p"], m["1m"], m["1fp"], m["1fm"]]
            for k, b, off, size_k in ((4, 0, 0, size), (5, 0, 0, size), (6, 3, 0, q), (7, 1, q, q)):
                r = slot(slice(0, A1_SENDS if name == "a1" else 4), b, off, size_k)
                sends.append(rc(r, r, ss.at[k], rs.at[4], up2))
            m["start"] = []
            for p in (0, 1):
                o, n_ = p * q, q
                m["start"].append([
                    rc(slot(0, 0, o, n_), slot(3, 0, o, n_), ss.at[0], rs.at[0], up1),
                    rc(slot(0, 0, o, n_), slot(1, 0, o, n_), ss.at[1], rs.at[1], dn1),
                    rc(slot(0, 0, o, n_), slot(0, 3, o, n_), ss.at[4], rs.at[4], up2),
                    rc(slot(0, 0, o, n_), slot(0, 1, o, n_), ss.at[5], rs.at[8], dn2)])
            m["sends"] = sends[:2] + sends[4:6] + [m["hp"], m["hm"]] if name == "a1" else sends
            halves.append(m)
        return halves

    R = {name: ring(name) for name in RINGS}

    def t0(name):
        l = int(name[1])
        if name == "a0":
            for p in (0, 1):
                for d in (1, 3):
                    xi_part(d, p).wait_recv()
                for k in range(4):
                    for m in R[name]:
                        m["start"][p][k].start()
            return
        if name[0] == "b":
            for h in (0, 1):
                xi2(l, h).wait_recv()
        for k in ("1p", "1m", ("2p", 0), ("2m", 0)):
            for m in R[name]:
                m[k].start()

    def t1(name):
        for k in "pm":
            for m in R[name]:
                m["1" + k].wait_recv()
            for m in R[name]:
                m["1f" + k].start()
        for e in (3, 1):
            for k in ("2p", "2m"):
                for m in R[name]:
                    m[k, e].start()

    def t2(name):
        for k in ("1fp", "1fm"):
            for m in R[name]:
                m[k].wait_recv()
        for k in ("2p", "2m"):
            for m in R[name]:
                m[k, 2].start()

    def t3(name, e):
        for k in "pm":
            for m in R[name]:
                m["2" + k, e].wait_recv()
            for m in R[name]:
                m["2f" + k, e].start()

    def t4(name, e):
        for k in ("2fp", "2fm"):
            for m in R[name]:
                m[k, e].wait_recv()

    def block(l, d, j, wt):
        src = X if l == 0 else Y1
        r = ((x + d) % NX) * per_x + c * half + j
        xs = [src[bi[l * (kk // T) + k, r]] for k in range(kk // T)]
        pre = jnp.dot(jnp.concatenate(xs, axis=1), wt, preferred_element_type=jnp.float32)
        pre = pre + bias[pl.ds(l, 1), pl.ds(pl.multiple_of(r * T, T), T)]
        act = jnp.maximum(pre, 0.0).astype(jnp.bfloat16)
        if l == 0:
            Y1[r] = act
        else:
            Ob[d, :, pl.ds(pl.multiple_of(j * T, T), T)] = act
        return act.astype(jnp.float32)

    def loop(l, n, step):
        def body(t, _):
            acc[l] = step(t, acc[l])
            return 0
        lax.fori_loop(0, n, body, 0)

    def own(l, lo=0, n=half):
        def step(t, s):
            for u in range(2):
                j = lo + t * 2 + u
                s = s + block(l, 0, j, Wo[l, j])
            return s
        loop(l, n // 2, step)

    def comp_a(l, n, fa, fb):
        def step(t, s):
            a, b = fa(t), fb(t)
            s = s + block(l, 1, place(a, b), Wb[l, 0, a, b])
            return s + block(l, 3, place(b, a), Wb[l, 2, b, a])
        loop(l, n, step)

    def comp_b(l, n, fa, fb):
        def step(t, s):
            a, b = fa(t), fb(t)
            s = s + block(l, 2, place(a, b), Wb[l, 1, a, b])
            return s + block(l, 2, place(b, a), Wb[l, 1, b, a])
        loop(l, n, step)

    def comp_b_rows(l, ey):
        def step(t, s):
            for u in range(2):
                s = s + block(l, 2, place(ey, t * 2 + u), Wb[l, 1, ey, t * 2 + u])
            return s
        loop(l, 2, step)

    def diag_b(l):
        def step(t, s):
            for u in range(2):
                e = t * 2 + u
                s = s + block(l, 2, place(e, e), Wb[l, 1, e, e])
            return s
        loop(l, 2, step)

    def osl(q):
        return pl.ds(pl.multiple_of(q * half * T, half * T), half * T)

    def y1x(d, other):
        ref = Y1.at[pl.ds((((x + d) % NX) * 2 + (c + other) % 2) * half, half)]
        return rc(ref, ref, y_ss.at[d], y_rs.at[d], dev(s=1))

    def out_send(d, s, j, n=1):
        src = Ob.at[d, xrow((c + s) % 2), pl.ds(pl.multiple_of(j * T, T), n * T)]
        dst = out.at[xrow(x), pl.ds(pl.multiple_of((c * half + j) * T, T), n * T)]
        if d == 0 and s == 0:
            return pltpu.make_async_copy(src, dst, l_sem.at[3])
        return rc(src, dst, o_ss.at[d, s], o_rs.at[d, s], dev(dx=d, s=s))

    def out_wait(d, s, recv):
        if recv:
            ref = out.at[xrow((x - d + NX) % NX), osl((c + s) % 2)]
            rc(ref, ref, o_ss.at[d, s], o_rs.at[d, s], dev(dx=d, s=s)).wait_recv()
        else:
            ref = Ob.at[d, xrow((c + s) % 2), :]
            rc(ref, ref, o_ss.at[d, s], o_rs.at[d, s], dev(dx=d, s=s)).wait_send()

    def send_a(pairs):
        for a, b in pairs:
            for s in (0, 1):
                out_send(1, s, place(a, b)).start()
                out_send(3, s, place(b, a)).start()

    def send_b(pairs):
        for a, b in pairs:
            for s in (0, 1):
                out_send(2, s, place(a, b)).start()

    def start_xi(l, ds):
        for d in ds:
            xi(l, d).start()

    acc[...] = jnp.zeros_like(acc)
    first[0].wait()
    for p in (0, 1):
        for d in (1, 3):
            xi_part(d, p).start()
    first[1].wait()
    start_xi(1, (1, 3))
    pltpu.make_async_copy(im, im, im_sem).wait()
    xf(0).start()
    mine_x = pltpu.make_async_copy(im.at[:, xrow(x), :], X.at[xblk(x), xrow(c), :], l_sem.at[5])
    mine_x.start()
    local.append(mine_x)

    t0("a0")
    for h in (0, 1):
        xi2(0, h).start()
    for d in (1, 3, 2):
        xa_send(d).start()
    t1("a0")
    for d in (1, 3):
        xi(1, d).wait_recv()
    for h in (0, 1):
        xi2(1, h).start()
    for cp in local:
        cp.wait()
    for k in range(NF):
        for h in (0, 1):
            far(h, k).start()
    t3("a0", 0)
    t0("b0")
    t2("a0")
    t3("a0", 3)
    t3("a0", 1)
    t1("b0")
    t3("a0", 2)
    t3("b0", 0)
    t2("b0")
    for d in (1, 3, 2):
        xa_recv(d).wait_recv()
        xf(d).start()
    t3("b0", 3)
    for d in (0, 1, 3, 2):
        xf(d, other=1).wait_recv()
    own(0)
    y1x(0, 0).start()
    t0("b1")
    t3("b0", 1)
    for e in range(4):
        t4("a0", e)
    comp_a(0, 4, lambda t: 0, lambda t: t)
    t3("b0", 2)
    comp_a(0, 4, lambda t: 1, lambda t: t)
    t1("b1")
    comp_a(0, 8, lambda t: 2 + t // 4, lambda t: t % 4)
    y1x(1, 0).start()
    y1x(3, 0).start()
    for e in range(4):
        t4("b0", e)
    for ey in range(4):
        comp_b_rows(0, ey)
    y1x(2, 0).start()
    t3("b1", 0)
    t2("b1")
    t0("a1")
    t3("b1", 3)
    t3("b1", 1)
    for d in range(4):
        y1x(d, 1).wait_recv()
    comp_b(1, 1, lambda t: 0, lambda t: 1)
    comp_b(1, 1, lambda t: 0, lambda t: 3)
    send_b([(0, 1), (1, 0), (0, 3), (3, 0)])
    t3("b1", 2)
    comp_b(1, 1, lambda t: 1, lambda t: 3)
    send_b([(1, 3), (3, 1)])
    for k in range(NF):
        for h in (0, 1):
            far(h, k).wait_recv()
    for k in ("hp", "hm"):
        for m in R["a1"]:
            m[k].start()
    comp_a(1, 2, lambda t: 2 * t, lambda t: 0)
    send_a([(0, 0), (2, 0)])
    comp_a(1, 4, lambda t: t, lambda t: 2)
    send_a([(0, 2), (1, 2), (2, 2), (3, 2)])
    for k in "pm":
        for m in R["a1"]:
            m["1" + k].wait_recv()
    for e in (3, 1):
        for k in ("2p", "2m"):
            for m in R["a1"]:
                m[k, e].start()
    for e in (0, 3, 1, 2):
        t4("b1", e)
    comp_b(1, 1, lambda t: 0, lambda t: 2)
    comp_b(1, 2, lambda t: 1 + 2 * t, lambda t: 2)
    diag_b(1)
    send_b([(0, 2), (2, 0), (0, 0), (1, 1), (2, 2), (3, 3), (1, 2), (2, 1), (3, 2), (2, 3)])
    comp_a(1, 2, lambda t: 1 + 2 * t, lambda t: 0)
    send_a([(1, 0), (3, 0)])
    for k in ("hp", "hm"):
        for m in R["a1"]:
            m[k].wait_recv()
    comp_a(1, 2, lambda t: 2, lambda t: 1 + 2 * t)
    send_a([(2, 1), (2, 3)])
    own(1)
    for s in (0, 1):
        out_send(0, s, 0, half).start()
    for e, ce in ((0, lambda t: 0), (3, lambda t: 3), (1, lambda t: 1)):
        for k in "pm":
            for m in R["a1"]:
                m["2" + k, e].wait_recv()
        comp_a(1, 2, ce, lambda t: 1 + 2 * t)
        send_a([(e, 1), (e, 3)])

    ax = rc(acc.at[:, xrow((c + 1) % 2), :], accr, a_ss.at[0], a_rs.at[0], dev(s=1))
    ax.start()
    mine = acc[:, xrow(c), :]
    ax.wait_recv()
    tot = jnp.sum(mine + accr[...], axis=2, keepdims=True)
    share = jnp.minimum(1.0, tot * (1.0 / (NX * cols * LIVE_LEVEL)))
    part_sum = jnp.broadcast_to(jnp.sum(share, axis=1, keepdims=True), (2, 1, T))

    def gather_sum(buf, n, me, val, targets, base):
        for l in range(2):
            buf[me, l:l + 1, :] = val[l]
        cps = [rc(buf.at[me], buf.at[me], z_ss.at[base + k], z_rs.at[base + k], t) for k, (t, _) in enumerate(targets)]
        for cp in cps:
            cp.start()
        for k, (_, who) in enumerate(targets):
            rc(buf.at[who], buf.at[who], z_ss.at[base + k], z_rs.at[base + k], dev(s=1)).wait_recv()
        total = jnp.sum(buf[...], axis=0)[:, None, :]
        return total, cps

    plane = [(dev(dy=a, dz=b), ((y - a + NY) % NY) * NZ + (z - b + NZ) % NZ)
             for b in (4, 3, 5, 2, 6, 1, 7, 0) for a in (2, 1, 3, 0) if a or b]
    v, cz = gather_sum(rz, NY * NZ, y * NZ + z, part_sum, plane, 0)
    me_x = [(dev(dx=d, s=s), ((x - d + NX) % NX) * 2 + (c + s) % 2) for d in (2, 1, 3, 0) for s in (0, 1) if d or s]
    v, cx = gather_sum(rx, 2 * NX, x * 2 + c, v, me_x, NY * NZ)
    v = v * (1.0 / (NX * rows * 2 * NZ * NY))
    for l in range(2):
        stat[l] = jnp.sum(v[l, 0:1, 0:1])

    for cp in cz + cx:
        cp.wait_send()
    for l in range(2):
        for d in (1, 3):
            xi(l, d).wait_send()
        for h in (0, 1):
            xi2(l, h).wait_send()
    for h in (0, 1):
        for k in range(len(FAR)):
            far(h, k).wait_send()
    for name in RINGS:
        for m in R[name]:
            for cp in m["sends"]:
                cp.wait_send()
    for d in (1, 2, 3):
        xa_send(d).wait_send()
    for d in range(4):
        xf(d).wait_send()
        y1x(d, 0).wait_send()
    ax.wait_send()
    out_send(0, 0, 0, half).wait()
    for d in range(4):
        for s in (0, 1):
            if d or s:
                out_wait(d, s, True)
                out_wait(d, s, False)


def per_device(images, weights, block_index, bias):
    n_img, cols = images.shape
    layers, per_x, kk, _ = weights.shape
    rows = n_img // NX
    half = per_x // 2
    total = cols * NX
    dma = pltpu.SemaphoreType.DMA
    any_ = pl.BlockSpec(memory_space=pl.ANY)
    index = jnp.transpose(block_index, (0, 2, 1)).reshape(layers * (kk // T), total // T)
    return pl.pallas_call(
        kernel,
        out_shape=(jax.ShapeDtypeStruct((n_img, cols), jnp.bfloat16), jax.ShapeDtypeStruct((layers,), jnp.float32)),
        in_specs=[any_] * 4,
        out_specs=(any_, pl.BlockSpec(memory_space=pltpu.SMEM)),
        scratch_shapes=[
            pltpu.VMEM((per_x, n_img, T), jnp.bfloat16),
            pltpu.VMEM((total // T, 2 * rows, T), jnp.bfloat16),
            pltpu.VMEM((total // T, 2 * rows, T), jnp.bfloat16),
            pltpu.VMEM((layers, 3, NY, NW, kk, T), jnp.bfloat16),
            pltpu.VMEM((layers, half, kk, T), jnp.bfloat16),
            pltpu.VMEM((NX, 2 * rows, half * T), jnp.bfloat16),
            pltpu.VMEM((layers, 2 * rows, T), jnp.float32),
            pltpu.VMEM((layers, rows, T), jnp.float32),
            pltpu.VMEM((NY * NZ, layers, T), jnp.float32),
            pltpu.VMEM((2 * NX, layers, T), jnp.float32),
            pltpu.SMEM(index.shape, jnp.int32),
            pltpu.VMEM(bias.shape, jnp.float32),
            pltpu.VMEM((layers, kk, T), jnp.bfloat16),
            dma((8,)), dma((8,)),
            dma((layers, 3)), dma((layers, 3)), dma((2, 2)), dma((layers, 2)), dma((layers, 2)),
            dma((2, 7)), dma((2, 7)),
            dma((4, 2, 8)), dma((4, 2, 20)),
            dma((4,)), dma((4,)),
            dma((4, 2)), dma((4, 2)),
            dma((1,)), dma((1,)),
            dma((6,)), dma, dma((2,)),
            dma((40,)), dma((40,)),
        ],
        compiler_params=pltpu.CompilerParams(collective_id=0, has_side_effects=True, vmem_limit_bytes=50 * 1024 * 1024),
        name="sparse_net",
    )(images, weights, index, bias)


def solution(mesh):
    return jax.shard_map(
        per_device, mesh=mesh,
        in_specs=(P("img", "nrn"), P(None, "nrn", None, None), P(), P()),
        out_specs=(P("img", "nrn"), P()), check_vma=False,
    )
```
